32 devices in a mesh: kv: 1 (over z), dup: 32 (over y, x, core).
Axes of the slice: x: 4, y: 4, z: 1, core: 2. Of those that a mesh axis runs over, the one named last changes fastest.
The devices are a block of a 4x4x8 slice.
Arguments:
- queries: bfloat16 [256, 64, 128], P('kv', 'dup')
- key_cache: bfloat16 [256, 4096, 128], P('kv', 'dup')
- value_cache: bfloat16 [256, 4096, 128], P('kv', 'dup')
- lengths: int32 [256], P('kv')
Outputs:
- output: bfloat16 [256, 64, 128], P('kv', 'dup')
All inputs are finite; a program needn't handle non-finite values.
Results may differ from the reference program's by a relative error of at most 0.00787467.
Values are sent between devices in bfloat16 or wider.
A program may use at most 768 MiB of HBM per device.

```python
import math
import jax
import jax.numpy as jnp
from jax import lax

BATCH = 256
SEQ = 4096
HEADS = 64
KV_HEADS = 4
HEAD_DIM = 128
DRAFT = 4

GROUP_HEADS = HEADS // KV_HEADS
QUERY_ROWS = GROUP_HEADS * DRAFT


def wave_field(k_freq, k_phase, k_dir, strength):
    spot_frac = jnp.arange(SEQ, dtype=jnp.float32) / SEQ
    freq_row = jax.random.randint(k_freq, (BATCH, 3), 1, 17, jnp.int32).astype(jnp.float32)
    phases = jax.random.uniform(k_phase, (BATCH, 3), jnp.float32) * (2.0 * math.pi)
    directions = jax.random.normal(k_dir, (BATCH, 3, HEAD_DIM), jnp.float32)
    wave_vals = jnp.cos(2.0 * math.pi * freq_row[:, None, :] * spot_frac[None, :, None] + phases[:, None, :])
    return strength * jnp.einsum("bsk,bkd->bsd", wave_vals, directions)


def setup_inputs(seed: int = 0, part: int = 0) -> dict:
    part_key = jax.random.fold_in(jax.random.key(seed), part)
    key_list = jax.random.split(part_key, 11)
    queries = jax.random.normal(key_list[0], (BATCH, QUERY_ROWS, HEAD_DIM), jnp.float32)
    k_noise = jax.random.normal(key_list[1], (BATCH, SEQ, HEAD_DIM), jnp.float32)
    key_cache = k_noise + wave_field(key_list[2], key_list[3], key_list[4], 1.5)
    v_noise = jax.random.normal(key_list[5], (BATCH, SEQ, HEAD_DIM), jnp.float32)
    value_cache = v_noise + wave_field(key_list[6], key_list[7], key_list[8], 1.0)
    low_len = max(DRAFT, SEQ // 8)
    lengths = jax.random.randint(key_list[9], (BATCH,), low_len, SEQ + 1, jnp.int32)
    full_row = jax.random.randint(key_list[10], (), 0, BATCH, jnp.int32)
    lengths = jnp.where(jnp.arange(BATCH) == full_row, SEQ, lengths).astype(jnp.int32)
    return {"queries": queries.astype(jnp.bfloat16), "key_cache": key_cache.astype(jnp.bfloat16), "value_cache": value_cache.astype(jnp.bfloat16), "lengths": lengths}


def reference(queries, key_cache, value_cache, lengths):
    score_scale = 1.0 / math.sqrt(HEAD_DIM)
    draft_pos = jnp.arange(QUERY_ROWS) % DRAFT
    seq_pos = jnp.arange(SEQ)

    def one_sequence(operands):
        q_rows, k_rows, v_rows, length = operands
        scores = jnp.dot(q_rows, k_rows.T, preferred_element_type=jnp.float32) * score_scale
        last_pos = length - DRAFT + draft_pos
        allowed = seq_pos[None, :] <= last_pos[:, None]
        scores = jnp.where(allowed, scores, -jnp.inf)
        row_peak = jnp.max(scores, axis=1, keepdims=True)
        prob_vals = jnp.exp(scores - row_peak)
        row_mass = jnp.sum(prob_vals, axis=1, keepdims=True)
        weighted = jnp.dot(prob_vals.astype(jnp.bfloat16), v_rows, preferred_element_type=jnp.float32)
        return (weighted / row_mass).astype(jnp.bfloat16)

    return lax.map(one_sequence, (queries, key_cache, value_cache, lengths))
```

```python
import functools
import math

import jax
import jax.numpy as jnp
from jax import lax
from jax.experimental import pallas as pl
from jax.experimental.pallas import tpu as pltpu
from jax.sharding import PartitionSpec as P

DRAFT = 4
CORES = 2
LANES = 128
TILE = 16
MASKED = -3.0e38
MESH = pl.DeviceIdType.MESH
F32 = jnp.float32
BF16 = jnp.bfloat16


def mixing(lams):
    top = functools.reduce(jnp.maximum, lams)
    parts = [jnp.exp2(lam - top) for lam in lams]
    total = functools.reduce(jnp.add, parts)
    inv = 1.0 / total
    return [part * inv for part in parts], top + jnp.log2(total)


def kernel(side, chunks, span, q_hbm, k_hbm, v_hbm, len_ref, out_ref,
           k_buf, v_buf, q_buf, o_buf, wt_buf,
           s0_o, s0_l, r0_o, r0_l, own_l,
           m0_o, m0_l, rel_o, rel_l, com_o, com_l, frm_o, frm_l,
           m1_o, m1_l, r1_o, r1_l,
           in_sem, ag1_s, ag1_r, ag2_s, ag2_r, agc_s, agc_r,
           rsc_s, rsc_r, rs2_s, rs2_r, rs1_s, rs1_r):
    seqs = q_buf.shape[1]
    rows = q_buf.shape[2] * q_buf.shape[3] * q_buf.shape[4] * q_buf.shape[5]
    own = q_buf.shape[5]
    head_dim = q_buf.shape[6]
    half_rows = rows // CORES
    pitch = o_buf.shape[1] // rows
    line = side * own
    hrow = line // 2

    me = lax.axis_index("dup")
    core = lax.rem(me, CORES)
    chip = me // CORES
    x, y = lax.rem(chip, side), chip // side
    a1 = x * (1 - core) + y * core
    a2 = y * (1 - core) + x * core
    step1 = (1 - core) + side * core
    step2 = side * (1 - core) + core

    def device(i1, i2):
        return (i1 * step1 + i2 * step2) * CORES + core

    def wrap(i):
        return lax.rem(i + side, side)

    twin = me + 1 - 2 * core
    right = device(a1, wrap(a2 + 1))
    left = device(a1, wrap(a2 - 1))
    peers = [device(wrap(a1 + d), a2) for d in range(1, side)]

    def send(src, dst, ssem, rsem, to):
        copy = pltpu.make_async_remote_copy(
            src_ref=src, dst_ref=dst, send_sem=ssem, recv_sem=rsem, device_id={"dup": to}, device_id_type=MESH)
        copy.start()
        return copy

    q_in = [pltpu.make_async_copy(q_hbm.at[pl.ds(k * seqs, seqs)], q_buf.at[k, :, 0, a2, a1], in_sem.at[0, k])
            for k in range(chunks)]
    kv_in = []
    for k in range(chunks):
        part = pl.ds(k * seqs, seqs)
        kv_in.append((pltpu.make_async_copy(k_hbm.at[part], k_buf.at[part], in_sem.at[1, k]),
                      pltpu.make_async_copy(v_hbm.at[part], v_buf.at[part], in_sem.at[2, k])))
    for copy in q_in:
        copy.start()
    for pair in kv_in:
        pair[0].start()
        pair[1].start()

    barrier = pltpu.get_barrier_semaphore()
    talk = [twin, right, left] + peers
    for dev in talk:
        pl.semaphore_signal(barrier, inc=1, device_id={"dup": dev}, device_id_type=MESH)
    pl.semaphore_wait(barrier, len(talk))

    sent = []
    got = {}

    def push(key, *args):
        copy = send(*args)
        sent.append(copy)
        got[key] = copy

    def gather1(k):
        q_in[k].wait()
        mine = q_buf.at[k, :, 0, a2, a1]
        for i, dev in enumerate(peers):
            push(("g1", k, i), mine, mine, ag1_s.at[k, i], ag1_r.at[k, i], dev)

    def gather2(k):
        for i in range(side - 1):
            got["g1", k, i].wait_recv()
        mine = q_buf.at[k, :, 0, a2]
        push(("g2", k, 0), mine, mine, ag2_s.at[k, 0], ag2_r.at[k, 0], right)
        push(("g2", k, 1), mine, mine, ag2_s.at[k, 1], ag2_r.at[k, 1], left)
        push(("gc", k, 0), mine, q_buf.at[k, :, 1, a2], agc_s.at[k, 0], agc_r.at[k, 0], twin)

    def gather3(k):
        mid = seqs // 2
        from_left, from_right = wrap(a2 - 1), wrap(a2 + 1)
        got["g2", k, 0].wait_recv()
        lo = q_buf.at[k, pl.ds(0, mid), 0, from_left]
        push(("g2", k, 2), lo, lo, ag2_s.at[k, 2], ag2_r.at[k, 2], right)
        push(("gc", k, 1), q_buf.at[k, :, 0, from_left], q_buf.at[k, :, 1, from_left],
             agc_s.at[k, 1], agc_r.at[k, 1], twin)
        got["g2", k, 1].wait_recv()
        hi = q_buf.at[k, pl.ds(mid, mid), 0, from_right]
        push(("g2", k, 3), hi, hi, ag2_s.at[k, 3], ag2_r.at[k, 3], left)
        push(("gc", k, 2), q_buf.at[k, :, 0, from_right], q_buf.at[k, :, 1, from_right],
             agc_s.at[k, 2], agc_r.at[k, 2], twin)

    def gather4(k):
        got["g2", k, 2].wait_recv()
        got["g2", k, 3].wait_recv()
        far = wrap(a2 + 2)
        push(("gc", k, 3), q_buf.at[k, :, 0, far], q_buf.at[k, :, 1, far], agc_s.at[k, 3], agc_r.at[k, 3], twin)

    def gather5(k):
        for i in range(side):
            got["gc", k, i].wait_recv()

    scale = (head_dim ** -0.5) * math.log2(math.e)

    def attend(k):
        kv_in[k][0].wait()
        kv_in[k][1].wait()
        row = lax.broadcasted_iota(jnp.int32, (rows, span), 0)
        lane = lax.broadcasted_iota(jnp.int32, (rows, span), 1)
        token = jnp.where(row < half_rows, core, 1 - core) * own + jnp.bitwise_and(row, own - 1)
        ahead = lane - token
        first = DRAFT + me * span
        seq_lane = lax.broadcasted_iota(jnp.int32, (rows, LANES), 1)
        slot = k % 2

        def step(b, lam):
            query = q_buf[k, b].reshape(rows, head_dim)
            s = lax.dot_general(query, k_buf[k * seqs + b], (((1,), (1,)), ((), ())), preferred_element_type=F32)
            s = jnp.where(ahead <= len_ref[k * seqs + b] - first, s, MASKED)
            top = jnp.max(s, axis=1, keepdims=True)
            p = jnp.exp2((s - top) * scale)
            mass = jnp.sum(p, axis=1, keepdims=True)
            o = jnp.dot(p.astype(BF16), v_buf[k * seqs + b], preferred_element_type=F32)
            o_buf[slot, pl.ds(b, rows, stride=pitch), :] = o * (1.0 / mass)
            return jnp.where(seq_lane == b, top * scale + jnp.log2(mass), lam)

        lam = lax.fori_loop(0, seqs, step, jnp.zeros((rows, LANES), F32), unroll=4)
        own_l[k] = lam[:half_rows]
        s0_l[k] = lam[half_rows:]

        def pack(t, carry):
            base = pl.multiple_of(t * TILE, TILE)
            for r in range(half_rows):
                s0_o[k, r, pl.ds(base, TILE), :] = o_buf[slot, pl.ds((half_rows + r) * pitch + base, TILE), :].astype(BF16)
            return carry

        lax.fori_loop(0, seqs // TILE, pack, 0)
        push(("c_l", k), s0_l.at[k], r0_l.at[k], rsc_s.at[k, 1], rsc_r.at[k, 1], twin)
        push(("c_o", k), s0_o.at[k], r0_o.at[k], rsc_s.at[k, 0], rsc_r.at[k, 0], twin)

    def turn(weights):
        stack = jnp.concatenate(weights, axis=0)
        if stack.shape[0] < LANES:
            stack = jnp.concatenate([stack, jnp.zeros((LANES - stack.shape[0], LANES), F32)], axis=0)
        wt_buf[...] = stack.T

    def blend(count, parts, store):
        def body(t, carry):
            base = pl.multiple_of(t * TILE, TILE)
            wt = wt_buf[pl.ds(base, TILE), :]
            for r in range(count):
                acc = None
                for i, part in enumerate(parts):
                    term = wt[:, i * count + r:i * count + r + 1] * part(r, base).astype(F32)
                    acc = term if acc is None else acc + term
                store(r, base, acc.astype(BF16))
            return carry

        lax.fori_loop(0, seqs // TILE, body, 0)

    def merge_core(k):
        got["c_l", k].wait_recv()
        got["c_o", k].wait_recv()
        weights, lam = mixing([own_l[k], r0_l[k]])
        for j in range(side):
            for h in range(2):
                m0_l[k, j, h] = lam[j * line + h * hrow:j * line + (h + 1) * hrow]
        turn(weights)
        slot = k % 2

        def store(r, base, value):
            m0_o[k, r // line, (r % line) // hrow, r % hrow, pl.ds(base, TILE), :] = value

        blend(half_rows,
              [lambda r, base: o_buf[slot, pl.ds(r * pitch + base, TILE), :],
               lambda r, base: r0_o[k, r, pl.ds(base, TILE), :]],
              store)
        far, next_, prev = wrap(a2 + 2), wrap(a2 + 1), wrap(a2 - 1)
        plan = [(far, 0, rel_o.at[k, 0], rel_l.at[k, 0], right),
                (far, 1, rel_o.at[k, 1], rel_l.at[k, 1], left),
                (next_, 1, frm_o.at[k, 0, 1], frm_l.at[k, 0, 1], right),
                (prev, 0, frm_o.at[k, 1, 0], frm_l.at[k, 1, 0], left)]
        for i, (j, h, dst_o, dst_l, to) in enumerate(plan):
            push(("2_l", k, i), m0_l.at[k, j, h], dst_l, rs2_s.at[k, i, 1], rs2_r.at[k, i, 1], to)
            push(("2_o", k, i), m0_o.at[k, j, h], dst_o, rs2_s.at[k, i, 0], rs2_r.at[k, i, 0], to)

    def relay(k):
        plan = [(wrap(a2 + 1), 0, right), (wrap(a2 - 1), 1, left)]
        for i, (j, h, to) in enumerate(plan):
            got["2_l", k, i].wait_recv()
            got["2_o", k, i].wait_recv()
            weights, lam = mixing([m0_l[k, j, h], rel_l[k, i]])
            com_l[k, i] = lam
            turn(weights)

            def store(r, base, value, i=i):
                com_o[k, i, r, pl.ds(base, TILE), :] = value

            blend(hrow,
                  [lambda r, base, j=j, h=h: m0_o[k, j, h, r, pl.ds(base, TILE), :],
                   lambda r, base, i=i: rel_o[k, i, r, pl.ds(base, TILE), :]],
                  store)
            push(("2_l", k, 4 + i), com_l.at[k, i], frm_l.at[k, i, i], rs2_s.at[k, 4 + i, 1], rs2_r.at[k, 4 + i, 1], to)
            push(("2_o", k, 4 + i), com_o.at[k, i], frm_o.at[k, i, i], rs2_s.at[k, 4 + i, 0], rs2_r.at[k, 4 + i, 0], to)

    def merge2(k):
        for i in range(2, 6):
            got["2_l", k, i].wait_recv()
            got["2_o", k, i].wait_recv()

        def whole(ref):
            return jnp.concatenate([ref[0], ref[1]], axis=0)

        weights, lam = mixing([whole(m0_l.at[k, a2]), whole(frm_l.at[k, 0]), whole(frm_l.at[k, 1])])
        for j in range(side):
            m1_l[k, j] = lam[j * own:(j + 1) * own]
        turn(weights)

        def store(r, base, value):
            m1_o[k, r // own, r % own, pl.ds(base, TILE), :] = value

        blend(line,
              [lambda r, base: m0_o[k, a2, r // hrow, r % hrow, pl.ds(base, TILE), :],
               lambda r, base: frm_o[k, 0, r // hrow, r % hrow, pl.ds(base, TILE), :],
               lambda r, base: frm_o[k, 1, r // hrow, r % hrow, pl.ds(base, TILE), :]],
              store)
        for i, dev in enumerate(peers):
            j = wrap(a1 + i + 1)
            push(("1_l", k, i), m1_l.at[k, j], r1_l.at[k, i], rs1_s.at[k, i, 1], rs1_r.at[k, i, 1], dev)
            push(("1_o", k, i), m1_o.at[k, j], r1_o.at[k, i], rs1_s.at[k, i, 0], rs1_r.at[k, i, 0], dev)

    def merge1(k):
        for i in range(side - 1):
            got["1_l", k, i].wait_recv()
            got["1_o", k, i].wait_recv()
        weights, _ = mixing([m1_l[k, a1]] + [r1_l[k, i] for i in range(side - 1)])
        turn(weights)

        def store(r, base, value):
            out_ref[r, pl.ds(k * seqs + base, TILE), :] = value

        blend(own,
              [lambda r, base: m1_o[k, a1, r, pl.ds(base, TILE), :]]
              + [lambda r, base, i=i: r1_o[k, i, r, pl.ds(base, TILE), :] for i in range(side - 1)],
              store)

    stages = {"g1": gather1, "g2": gather2, "g3": gather3, "g4": gather4, "g5": gather5,
              "at": attend, "mc": merge_core, "rl": relay, "m2": merge2, "m1": merge1}
    for name, k in order(chunks):
        stages[name](k)
    for copy in sent:
        copy.wait_send()


def order(chunks):
    plan = [("g1", k) for k in range(chunks)]
    ticks = []
    lag = {"g2": 0, "g3": 2, "g4": 3, "g5": 4, "at": 4, "mc": 5, "rl": 6, "m2": 7, "m1": 8}
    rank = {"g2": 2, "g3": 0, "g4": 1, "mc": 3, "rl": 4, "m2": 5, "m1": 6, "g5": 7, "at": 8}
    for k in range(chunks):
        for name, late in lag.items():
            ticks.append((k + late, rank[name], k, name))
    return plan + [(name, k) for _, _, k, name in sorted(ticks)]


def solution(mesh):
    dup_size = mesh.shape["dup"]
    side = math.isqrt(dup_size // CORES)
    chunks = 4

    def group_step(q_local, k_span, v_span, len_local):
        num_batch, span, head_dim = k_span.shape
        own = q_local.shape[1]
        rows = own * dup_size
        half_rows = rows // CORES
        line = side * own
        hrow = line // 2
        seqs = num_batch // chunks
        pitch = seqs + 8
        vm = pltpu.VMEM
        dma = pltpu.SemaphoreType.DMA
        out = pl.pallas_call(
            functools.partial(kernel, side, chunks, span),
            out_shape=jax.ShapeDtypeStruct((own, num_batch, head_dim), BF16),
            in_specs=[pl.BlockSpec(memory_space=pl.ANY)] * 3 + [pl.BlockSpec(memory_space=pltpu.SMEM)],
            out_specs=pl.BlockSpec(memory_space=pltpu.VMEM),
            scratch_shapes=[
                vm((num_batch, span, head_dim), BF16), vm((num_batch, span, head_dim), BF16),
                vm((chunks, seqs, CORES, side, side, own, head_dim), BF16),
                vm((2, rows * pitch, head_dim), F32), vm((LANES, LANES), F32),
                vm((chunks, half_rows, seqs, head_dim), BF16), vm((chunks, half_rows, LANES), F32),
                vm((chunks, half_rows, seqs, head_dim), BF16), vm((chunks, half_rows, LANES), F32),
                vm((chunks, half_rows, LANES), F32),
                vm((chunks, side, 2, hrow, seqs, head_dim), BF16), vm((chunks, side, 2, hrow, LANES), F32),
                vm((chunks, 2, hrow, seqs, head_dim), BF16), vm((chunks, 2, hrow, LANES), F32),
                vm((chunks, 2, hrow, seqs, head_dim), BF16), vm((chunks, 2, hrow, LANES), F32),
                vm((chunks, 2, 2, hrow, seqs, head_dim), BF16), vm((chunks, 2, 2, hrow, LANES), F32),
                vm((chunks, side, own, seqs, head_dim), BF16), vm((chunks, side, own, LANES), F32),
                vm((chunks, side - 1, own, seqs, head_dim), BF16), vm((chunks, side - 1, own, LANES), F32),
                dma((3, chunks)),
                dma((chunks, side - 1)), dma((chunks, side - 1)),
                dma((chunks, 4)), dma((chunks, 4)),
                dma((chunks, side)), dma((chunks, side)),
                dma((chunks, 2)), dma((chunks, 2)),
                dma((chunks, 6, 2)), dma((chunks, 6, 2)),
                dma((chunks, side - 1, 2)), dma((chunks, side - 1, 2)),
            ],
            compiler_params=pltpu.CompilerParams(
                collective_id=0, has_side_effects=True, vmem_limit_bytes=60 * 1024 * 1024),
            name="decode_group",
        )(q_local, k_span, v_span, len_local)
        return jnp.swapaxes(out, 0, 1)

    return jax.shard_map(group_step, mesh=mesh, in_specs=(P("kv", "dup", None), P("kv", "dup", None), P("kv", "dup", None), P("kv")), out_specs=P("kv", "dup", None), check_vma=False)
```

```python
import functools
import math

import jax
import jax.numpy as jnp
from jax import lax
from jax.experimental import pallas as pl
from jax.experimental.pallas import tpu as pltpu
from jax.sharding import PartitionSpec as P

DRAFT = 4
CORES = 2
LANES = 128
TILE = 16
GROUP = 8
MASKED = -3.0e38
MESH = pl.DeviceIdType.MESH
F32 = jnp.float32
BF16 = jnp.bfloat16


def mixing(lams, masses=None):
    top = functools.reduce(jnp.maximum, lams)
    parts = [jnp.exp2(lam - top) for lam in lams]
    masses = parts if masses is None else [part * mass for part, mass in zip(parts, masses)]
    total = functools.reduce(jnp.add, masses)
    inv = 1.0 / total
    return [part * inv for part in parts], top + jnp.log2(total)


def kernel(side, chunks, span, q_hbm, k_hbm, v_hbm, len_ref, out_ref,
           k_buf, v_buf, q_buf, o_buf, wt_buf, s_buf, p_buf, top_buf, mass_buf,
           s0_o, s0_l, r0_o, r0_l, own_l,
           m0_o, m0_l, rel_o, rel_l, com_o, com_l, frm_o, frm_l,
           m1_o, m1_l, r1_o, r1_l,
           in_sem, ag1_s, ag1_r, ag2_s, ag2_r, agc_s, agc_r,
           rsc_s, rsc_r, rs2_s, rs2_r, rs1_s, rs1_r):
    seqs = q_buf.shape[1]
    rows = q_buf.shape[2] * q_buf.shape[3] * q_buf.shape[4] * q_buf.shape[5]
    own = q_buf.shape[5]
    head_dim = q_buf.shape[6]
    half_rows = rows // CORES
    pitch = o_buf.shape[1] // rows
    line = side * own
    hrow = line // 2

    q_flat = q_buf.reshape(q_buf.shape[0], seqs, rows, head_dim)

    me = lax.axis_index("dup")
    core = lax.rem(me, CORES)
    chip = me // CORES
    x, y = lax.rem(chip, side), chip // side
    a1 = x * (1 - core) + y * core
    a2 = y * (1 - core) + x * core
    step1 = (1 - core) + side * core
    step2 = side * (1 - core) + core

    def device(i1, i2):
        return (i1 * step1 + i2 * step2) * CORES + core

    def wrap(i):
        return lax.rem(i + side, side)

    twin = me + 1 - 2 * core
    right = device(a1, wrap(a2 + 1))
    left = device(a1, wrap(a2 - 1))
    peers = [device(wrap(a1 + d), a2) for d in range(1, side)]

    def send(src, dst, ssem, rsem, to):
        copy = pltpu.make_async_remote_copy(
            src_ref=src, dst_ref=dst, send_sem=ssem, recv_sem=rsem, device_id={"dup": to}, device_id_type=MESH)
        copy.start()
        return copy

    q_in = [pltpu.make_async_copy(q_hbm.at[pl.ds(k * seqs, seqs)], q_buf.at[k, :, 0, a2, a1], in_sem.at[0, k])
            for k in range(chunks)]
    kv_in = []
    for k in range(chunks):
        part = pl.ds(k * seqs, seqs)
        kv_in.append((pltpu.make_async_copy(k_hbm.at[part], k_buf.at[part], in_sem.at[1, k]),
                      pltpu.make_async_copy(v_hbm.at[part], v_buf.at[part], in_sem.at[2, k])))
    for copy in q_in:
        copy.start()
    for pair in kv_in:
        pair[0].start()
        pair[1].start()

    barrier = pltpu.get_barrier_semaphore()
    talk = [twin, right, left] + peers
    for dev in talk:
        pl.semaphore_signal(barrier, inc=1, device_id={"dup": dev}, device_id_type=MESH)
    with jax.named_scope("barrier"):
        pl.semaphore_wait(barrier, len(talk))

    sent = []
    got = {}

    def push(key, *args):
        copy = send(*args)
        sent.append(copy)
        got[key] = copy

    def gather1(k):
        q_in[k].wait()
        mine = q_buf.at[k, :, 0, a2, a1]
        for i, dev in enumerate(peers):
            push(("g1", k, i), mine, mine, ag1_s.at[k, i], ag1_r.at[k, i], dev)

    def gather2(k):
        for i in range(side - 1):
            got["g1", k, i].wait_recv()
        mine = q_buf.at[k, :, 0, a2]
        push(("g2", k, 0), mine, mine, ag2_s.at[k, 0], ag2_r.at[k, 0], right)
        push(("g2", k, 1), mine, mine, ag2_s.at[k, 1], ag2_r.at[k, 1], left)
        push(("gc", k, 0), mine, q_buf.at[k, :, 1, a2], agc_s.at[k, 0], agc_r.at[k, 0], twin)

    def gather3(k):
        mid = seqs // 2
        from_left, from_right = wrap(a2 - 1), wrap(a2 + 1)
        got["g2", k, 0].wait_recv()
        lo = q_buf.at[k, pl.ds(0, mid), 0, from_left]
        push(("g2", k, 2), lo, lo, ag2_s.at[k, 2], ag2_r.at[k, 2], right)
        push(("gc", k, 1), q_buf.at[k, :, 0, from_left], q_buf.at[k, :, 1, from_left],
             agc_s.at[k, 1], agc_r.at[k, 1], twin)
        got["g2", k, 1].wait_recv()
        hi = q_buf.at[k, pl.ds(mid, mid), 0, from_right]
        push(("g2", k, 3), hi, hi, ag2_s.at[k, 3], ag2_r.at[k, 3], left)
        push(("gc", k, 2), q_buf.at[k, :, 0, from_right], q_buf.at[k, :, 1, from_right],
             agc_s.at[k, 2], agc_r.at[k, 2], twin)

    def gather4(k):
        got["g2", k, 2].wait_recv()
        got["g2", k, 3].wait_recv()
        far = wrap(a2 + 2)
        push(("gc", k, 3), q_buf.at[k, :, 0, far], q_buf.at[k, :, 1, far], agc_s.at[k, 3], agc_r.at[k, 3], twin)

    def gather5(k):
        for i in range(side):
            got["gc", k, i].wait_recv()

    scale = (head_dim ** -0.5) * math.log2(math.e)

    def attend(k):
        kv_in[k][0].wait()
        kv_in[k][1].wait()
        first = DRAFT + me * span
        slot = k % 2
        groups = seqs // GROUP

        def step(i, carry):
            g = lax.rem(i + groups - 2, groups) * GROUP
            for u in range(GROUP):
                p = p_buf[u * rows:(u + 1) * rows, :]
                o = jnp.dot(p, v_buf[k * seqs + g + u], preferred_element_type=F32)
                o_buf[slot, pl.ds(g + u, rows, stride=pitch), :] = o
            g = lax.rem(i + groups - 1, groups) * GROUP
            row = lax.broadcasted_iota(jnp.int32, (rows, span), 0)
            lane = lax.broadcasted_iota(jnp.int32, (rows, span), 1)
            token = jnp.where(row < half_rows, core, 1 - core) * own + jnp.bitwise_and(row, own - 1)
            ahead = lane - token
            seq_lane = lax.broadcasted_iota(jnp.int32, (rows, LANES), 1)
            tops, masses = top_buf[...], mass_buf[...]
            for u in range(GROUP):
                s = s_buf[u * rows:(u + 1) * rows, :]
                s = jnp.where(ahead <= len_ref[k * seqs + g + u] - first, s, MASKED)
                top = jnp.max(s, axis=1, keepdims=True)
                p = jnp.exp2((s - top) * scale)
                mass = jnp.sum(p, axis=1, keepdims=True)
                p_buf[u * rows:(u + 1) * rows, :] = p.astype(BF16)
                tops = jnp.where(seq_lane == g + u, top, tops)
                masses = jnp.where(seq_lane == g + u, mass, masses)
            top_buf[...] = tops
            mass_buf[...] = masses
            g = lax.rem(i, groups) * GROUP
            for u in range(GROUP):
                s_buf[u * rows:(u + 1) * rows, :] = lax.dot_general(
                    q_flat[k, g + u], k_buf[k * seqs + g + u], (((1,), (1,)), ((), ())), preferred_element_type=F32)
            return carry

        with jax.named_scope("loop"):
            lax.fori_loop(0, groups + 2, step, 0)
        for h, ref in enumerate((own_l, s0_l)):
            ref[k, 0] = top_buf[h * half_rows:(h + 1) * half_rows, :] * scale
            ref[k, 1] = mass_buf[h * half_rows:(h + 1) * half_rows, :]

        def pack(t, carry):
            base = pl.multiple_of(t * TILE, TILE)
            for r in range(half_rows):
                s0_o[k, r, pl.ds(base, TILE), :] = o_buf[slot, pl.ds((half_rows + r) * pitch + base, TILE), :].astype(BF16)
            return carry

        lax.fori_loop(0, seqs // TILE, pack, 0)
        push(("c_l", k), s0_l.at[k], r0_l.at[k], rsc_s.at[k, 1], rsc_r.at[k, 1], twin)
        push(("c_o", k), s0_o.at[k], r0_o.at[k], rsc_s.at[k, 0], rsc_r.at[k, 0], twin)

    def turn(weights):
        stack = jnp.concatenate(weights, axis=0)
        if stack.shape[0] < LANES:
            stack = jnp.concatenate([stack, jnp.zeros((LANES - stack.shape[0], LANES), F32)], axis=0)
        wt_buf[...] = stack.T

    def blend(count, parts, store):
        def body(t, carry):
            base = pl.multiple_of(t * TILE, TILE)
            wt = wt_buf[pl.ds(base, TILE), :]
            for r in range(count):
                acc = None
                for i, part in enumerate(parts):
                    term = wt[:, i * count + r:i * count + r + 1] * part(r, base).astype(F32)
                    acc = term if acc is None else acc + term
                store(r, base, acc.astype(BF16))
            return carry

        lax.fori_loop(0, seqs // TILE, body, 0)

    def merge_core(k):
        with jax.named_scope("wait"):
            got["c_l", k].wait_recv()
            got["c_o", k].wait_recv()
        weights, lam = mixing([own_l[k, 0], r0_l[k, 0]], [own_l[k, 1], r0_l[k, 1]])
        for j in range(side):
            for h in range(2):
                m0_l[k, j, h] = lam[j * line + h * hrow:j * line + (h + 1) * hrow]
        turn(weights)
        slot = k % 2

        def store(r, base, value):
            m0_o[k, r // line, (r % line) // hrow, r % hrow, pl.ds(base, TILE), :] = value

        blend(half_rows,
              [lambda r, base: o_buf[slot, pl.ds(r * pitch + base, TILE), :],
               lambda r, base: r0_o[k, r, pl.ds(base, TILE), :]],
              store)
        far, next_, prev = wrap(a2 + 2), wrap(a2 + 1), wrap(a2 - 1)
        plan = [(far, 0, rel_o.at[k, 0], rel_l.at[k, 0], right),
                (far, 1, rel_o.at[k, 1], rel_l.at[k, 1], left),
                (next_, 1, frm_o.at[k, 0, 1], frm_l.at[k, 0, 1], right),
                (prev, 0, frm_o.at[k, 1, 0], frm_l.at[k, 1, 0], left)]
        for i, (j, h, dst_o, dst_l, to) in enumerate(plan):
            push(("2_l", k, i), m0_l.at[k, j, h], dst_l, rs2_s.at[k, i, 1], rs2_r.at[k, i, 1], to)
            push(("2_o", k, i), m0_o.at[k, j, h], dst_o, rs2_s.at[k, i, 0], rs2_r.at[k, i, 0], to)

    def relay(k):
        plan = [(wrap(a2 + 1), 0, right), (wrap(a2 - 1), 1, left)]
        for i, (j, h, to) in enumerate(plan):
            with jax.named_scope("wait"):
                got["2_l", k, i].wait_recv()
                got["2_o", k, i].wait_recv()
            weights, lam = mixing([m0_l[k, j, h], rel_l[k, i]])
            com_l[k, i] = lam
            turn(weights)

            def store(r, base, value, i=i):
                com_o[k, i, r, pl.ds(base, TILE), :] = value

            blend(hrow,
                  [lambda r, base, j=j, h=h: m0_o[k, j, h, r, pl.ds(base, TILE), :],
                   lambda r, base, i=i: rel_o[k, i, r, pl.ds(base, TILE), :]],
                  store)
            push(("2_l", k, 4 + i), com_l.at[k, i], frm_l.at[k, i, i], rs2_s.at[k, 4 + i, 1], rs2_r.at[k, 4 + i, 1], to)
            push(("2_o", k, 4 + i), com_o.at[k, i], frm_o.at[k, i, i], rs2_s.at[k, 4 + i, 0], rs2_r.at[k, 4 + i, 0], to)

    def merge2(k):
        with jax.named_scope("wait"):
            for i in range(2, 6):
                got["2_l", k, i].wait_recv()
                got["2_o", k, i].wait_recv()

        def whole(ref):
            return jnp.concatenate([ref[0], ref[1]], axis=0)

        weights, lam = mixing([whole(m0_l.at[k, a2]), whole(frm_l.at[k, 0]), whole(frm_l.at[k, 1])])
        for j in range(side):
            m1_l[k, j] = lam[j * own:(j + 1) * own]
        turn(weights)

        def store(r, base, value):
            m1_o[k, r // own, r % own, pl.ds(base, TILE), :] = value

        blend(line,
              [lambda r, base: m0_o[k, a2, r // hrow, r % hrow, pl.ds(base, TILE), :],
               lambda r, base: frm_o[k, 0, r // hrow, r % hrow, pl.ds(base, TILE), :],
               lambda r, base: frm_o[k, 1, r // hrow, r % hrow, pl.ds(base, TILE), :]],
              store)
        for i, dev in enumerate(peers):
            j = wrap(a1 + i + 1)
            push(("1_l", k, i), m1_l.at[k, j], r1_l.at[k, i], rs1_s.at[k, i, 1], rs1_r.at[k, i, 1], dev)
            push(("1_o", k, i), m1_o.at[k, j], r1_o.at[k, i], rs1_s.at[k, i, 0], rs1_r.at[k, i, 0], dev)

    def merge1(k):
        with jax.named_scope("wait"):
            for i in range(side - 1):
                got["1_l", k, i].wait_recv()
                got["1_o", k, i].wait_recv()
        weights, _ = mixing([m1_l[k, a1]] + [r1_l[k, i] for i in range(side - 1)])
        turn(weights)

        def store(r, base, value):
            out_ref[r, pl.ds(k * seqs + base, TILE), :] = value

        blend(own,
              [lambda r, base: m1_o[k, a1, r, pl.ds(base, TILE), :]]
              + [lambda r, base, i=i: r1_o[k, i, r, pl.ds(base, TILE), :] for i in range(side - 1)],
              store)

    stages = {"g1": gather1, "g2": gather2, "g3": gather3, "g4": gather4, "g5": gather5,
              "at": attend, "mc": merge_core, "rl": relay, "m2": merge2, "m1": merge1}
    for name, k in order(chunks):
        with jax.named_scope(f"{name}_{k}"):
            stages[name](k)
    with jax.named_scope("drain"):
        for copy in sent:
            copy.wait_send()


def order(chunks):
    plan = [("g1", k) for k in range(chunks)]
    ticks = []
    lag = {"g2": 0, "g3": 2, "g4": 3, "g5": 4, "at": 4, "mc": 6, "rl": 7, "m2": 8, "m1": 9}
    rank = {"g2": 2, "g3": 0, "g4": 1, "mc": 3, "rl": 4, "m2": 5, "m1": 6, "g5": 7, "at": 8}
    for k in range(chunks):
        for name, late in lag.items():
            ticks.append((k + late, rank[name], k, name))
    return plan + [(name, k) for _, _, k, name in sorted(ticks)]


def solution(mesh):
    dup_size = mesh.shape["dup"]
    side = math.isqrt(dup_size // CORES)
    chunks = 4

    def group_step(q_local, k_span, v_span, len_local):
        num_batch, span, head_dim = k_span.shape
        own = q_local.shape[1]
        rows = own * dup_size
        half_rows = rows // CORES
        line = side * own
        hrow = line // 2
        seqs = num_batch // chunks
        pitch = seqs + 8
        vm = pltpu.VMEM
        dma = pltpu.SemaphoreType.DMA
        out = pl.pallas_call(
            functools.partial(kernel, side, chunks, span),
            out_shape=jax.ShapeDtypeStruct((own, num_batch, head_dim), BF16),
            in_specs=[pl.BlockSpec(memory_space=pl.ANY)] * 3 + [pl.BlockSpec(memory_space=pltpu.SMEM)],
            out_specs=pl.BlockSpec(memory_space=pltpu.VMEM),
            scratch_shapes=[
                vm((num_batch, span, head_dim), BF16), vm((num_batch, span, head_dim), BF16),
                vm((chunks, seqs, CORES, side, side, own, head_dim), BF16),
                vm((2, rows * pitch, head_dim), F32), vm((LANES, LANES), F32),
                vm((GROUP * rows, span), F32), vm((GROUP * rows, span), BF16),
                vm((rows, LANES), F32), vm((rows, LANES), F32),
                vm((chunks, half_rows, seqs, head_dim), BF16), vm((chunks, 2, half_rows, LANES), F32),
                vm((chunks, half_rows, seqs, head_dim), BF16), vm((chunks, 2, half_rows, LANES), F32),
                vm((chunks, 2, half_rows, LANES), F32),
                vm((chunks, side, 2, hrow, seqs, head_dim), BF16), vm((chunks, side, 2, hrow, LANES), F32),
                vm((chunks, 2, hrow, seqs, head_dim), BF16), vm((chunks, 2, hrow, LANES), F32),
                vm((chunks, 2, hrow, seqs, head_dim), BF16), vm((chunks, 2, hrow, LANES), F32),
                vm((chunks, 2, 2, hrow, seqs, head_dim), BF16), vm((chunks, 2, 2, hrow, LANES), F32),
                vm((chunks, side, own, seqs, head_dim), BF16), vm((chunks, side, own, LANES), F32),
                vm((chunks, side - 1, own, seqs, head_dim), BF16), vm((chunks, side - 1, own, LANES), F32),
                dma((3, chunks)),
                dma((chunks, side - 1)), dma((chunks, side - 1)),
                dma((chunks, 4)), dma((chunks, 4)),
                dma((chunks, side)), dma((chunks, side)),
                dma((chunks, 2)), dma((chunks, 2)),
                dma((chunks, 6, 2)), dma((chunks, 6, 2)),
                dma((chunks, side - 1, 2)), dma((chunks, side - 1, 2)),
            ],
            compiler_params=pltpu.CompilerParams(
                collective_id=0, has_side_effects=True, vmem_limit_bytes=60 * 1024 * 1024),
            name="decode_group",
        )(q_local, k_span, v_span, len_local)
        return jnp.swapaxes(out, 0, 1)

    return jax.shard_map(group_step, mesh=mesh, in_specs=(P("kv", "dup", None), P("kv", "dup", None), P("kv", "dup", None), P("kv")), out_specs=P("kv", "dup", None), check_vma=False)
```
